256 devices in a mesh: rows: 16 (over y, x_lo, core), cols: 4 (over z_1, x_hi), slabs: 2 (over z_0), trial: 2 (over z_2).
Axes of the slice: x: 4 (x_hi: 2, x_lo: 2; x = x_hi * 2 + x_lo), y: 4, z: 8 (z_0: 2, z_1: 2, z_2: 2; z = z_0 * 4 + z_1 * 2 + z_2), core: 2. Of those that a mesh axis runs over, the one named last changes fastest.
Arguments:
- field_values: float32 [256, 64, 128, 128], P(('trial', 'rows'), 'cols', 'slabs'), parts along dimension 0, may hold values from 0.2 to 1.8
- crowding: float32 [256, 64, 128, 128], P(('trial', 'rows'), 'cols', 'slabs'), parts along dimension 0, may hold values from 0.5 to 2
Outputs:
- potential: float32 [256, 64, 128, 128], P(('trial', 'rows'), 'cols', 'slabs'), parts along dimension 0
- field_values_end: float32 [256, 64, 128, 128], P(('trial', 'rows'), 'cols', 'slabs'), parts along dimension 0
The draws below stay inside these ranges and needn't reach their ends.
There are 2 independent parts, one for each index of `trial`. The reference program is written for one: setup_inputs(seed, part) draws one part's arguments, and reference() takes and returns one part's arrays. A program takes and returns all parts, laid end to end along the dimension named above; each array names one. Nothing has to cross between parts.
All inputs are finite; a program needn't handle non-finite values.
Results may differ from the reference program's by a relative error of at most 0.00002.
Values sent between devices are 32-bit elements; how exact they have to be, the bound alone decides.
A program may use at most 64 MiB of HBM per device.

```python
import jax
import jax.numpy as jnp
from jax import lax

GRID_J = 128
GRID_I = 64
GRID_K = 128
LEVELS = 128
STEPS = 3


def block_levels(rng, shape, pieces, least, top_value):
    factor_of = 1.0
    for axis_at, parts in pieces:
        steps = jax.random.uniform(jax.random.fold_in(jax.random.fold_in(rng, 6), axis_at), (parts,), jnp.float32, least / len(pieces), top_value / len(pieces))
        factor_of = factor_of * jnp.repeat(jnp.exp(steps), shape[axis_at] // parts).reshape((-1,) + (1,) * (len(shape) - 1 - axis_at))
    return factor_of


def setup_inputs(seed: int = 0, part: int = 0) -> dict:
    keys = jax.random.split(jax.random.key(seed), 3)
    part_splits = jax.random.split(jax.random.fold_in(keys[2], part), 3)
    return {
        "field_values": jnp.clip(0.2 + 1.5999999 * jax.random.uniform(part_splits[0], (GRID_J, GRID_I, GRID_K, LEVELS), jnp.float32) ** block_levels(part_splits[0], (GRID_J, GRID_I, GRID_K, LEVELS), ((0, 16), (1, 4), (2, 2)), -0.2, 0.2), 0.2, 1.8),
        "crowding": jnp.clip(0.5 + 1.5 * jax.random.uniform(part_splits[1], (GRID_J, GRID_I, GRID_K, LEVELS), jnp.float32) ** block_levels(part_splits[1], (GRID_J, GRID_I, GRID_K, LEVELS), ((0, 16), (1, 4), (2, 2)), -0.2, 0.2), 0.5, 2.0),
    }


def without_rim(values, dims):
    for dim in dims:
        values = lax.slice_in_dim(values, 1, values.shape[dim] - 1, axis=dim)
    return values


def shifted_cells(values, dim, start, dims):
    others = [other for other in dims if other != dim]
    values = without_rim(values, others)
    return lax.slice_in_dim(values, start, start + values.shape[dim] - 2, axis=dim)


def march_step(padded, crowding):
    middle = without_rim(padded, (0, 1, 2))
    lower = [shifted_cells(padded, dim, 0, (0, 1, 2)) for dim in (0, 1, 2)]
    upper = [shifted_cells(padded, dim, 2, (0, 1, 2)) for dim in (0, 1, 2)]
    spread = lower[0] + upper[0] + lower[1] + upper[1] + lower[2] + upper[2] - 6.0 * middle
    return middle + 0.1 * spread + 0.2 * middle * (1.0 - middle * crowding)


def reference(field_values, crowding):
    for step in range(STEPS):
        field_values = march_step(jnp.pad(field_values, ((1, 1), (1, 1), (1, 1), (0, 0)), mode="constant"), crowding)
    potential = jnp.cumsum(field_values, axis=0) / GRID_J
    return potential, field_values
```

```python
import functools

import jax
import jax.numpy as jnp
from jax import lax
from jax.experimental import pallas as pl
from jax.experimental.pallas import tpu as pltpu
from jax.sharding import PartitionSpec as P

MESH = pl.DeviceIdType.MESH
F32 = jnp.float32
STEPS = 3
NJ, NI, NK, NL = 8, 16, 64, 128
K0 = 8
EDGE = ((0, 4), (12, 4))
MID = ((4, 8),)
GROUPS = EDGE + MID
CELLS = pl.ds(K0, NK)
N_SEM = 12
UP, DOWN, I_UP, I_DOWN, KF = 0, 3, 6, 7, 8


def rows_of(groups, body):
    for start, count in groups:
        lax.fori_loop(start, start + count, lambda i, _: (body(i), 0)[1], 0)


def exchange_kernel(fv, cr, out, below, u0, u1, u2, c, kf, kh, tot, tot_p, x_in, x_out, p_in, z, z_p, load_sem, s_sem, r_sem, ps_sem, pr_sem):
    r, col, slab = lax.axis_index("rows"), lax.axis_index("cols"), lax.axis_index("slabs")
    core = lax.rem(r, 2)
    x_lo = lax.rem(lax.div(r, 2), 2)
    y = lax.div(r, 4)
    u = (u0, u1, u2)
    other_core = {"rows": r + 1 - 2 * core}
    other_chip = {"rows": r + 2 - 4 * x_lo}

    has = {UP: r < 15, DOWN: r > 0, I_UP: col < 3, I_DOWN: col > 0}
    to = {UP: {"rows": r + 1}, DOWN: {"rows": r - 1}, I_UP: {"cols": col + 1}, I_DOWN: {"cols": col - 1}}
    barrier = pltpu.get_barrier_semaphore()
    count = jnp.int32(2)
    for way in (UP, DOWN, I_UP, I_DOWN):
        count = count + jnp.where(has[way], 1, 0)

        @pl.when(has[way])
        def _(way=way):
            pl.semaphore_signal(barrier, 1, device_id=to[way], device_id_type=MESH)

    for ok, dst in ((y < 3, {"rows": r + 4}), (y > 0, {"rows": r - 4})):
        count = count + jnp.where(ok, 1, 0)

        @pl.when(ok)
        def _(dst=dst):
            pl.semaphore_signal(barrier, 1, device_id=dst, device_id_type=MESH)

    pl.semaphore_signal(barrier, 1, device_id={"slabs": 1 - slab}, device_id_type=MESH)
    pl.semaphore_signal(barrier, 1, device_id=other_chip, device_id_type=MESH)

    load_u = pltpu.make_async_copy(fv, u0.at[pl.ds(1, NJ), pl.ds(1, NI), CELLS], load_sem.at[0])
    load_c = pltpu.make_async_copy(cr, c, load_sem.at[1])
    load_u.start()
    load_c.start()

    edge_row = jnp.where(slab == 0, K0 - 1, K0 + NK)
    halo_row = jnp.where(slab == 0, K0 + NK, K0 - 1)
    face_row = jnp.where(slab == 0, K0 + NK - 1, K0)
    zero_plane = jnp.zeros((NK, NL), F32)
    zero_line = jnp.zeros((1, NL), F32)

    def zero_lines(i):
        for b in u:
            for j in range(NJ):
                b[j + 1, i + 1, pl.ds(edge_row, 1), :] = zero_line

    rows_of(((0, NI),), zero_lines)

    def zero_j(plane):
        def body(i):
            for b in u:
                b[plane, i + 1, CELLS, :] = zero_plane

        rows_of(((0, NI),), body)

    def zero_i(row):
        def body(j):
            for b in u:
                b[j + 1, row, CELLS, :] = zero_plane

        rows_of(((0, NJ),), body)

    pl.when(r == 0)(lambda: zero_j(0))
    pl.when(r == 15)(lambda: zero_j(NJ + 1))
    pl.when(col == 0)(lambda: zero_i(0))
    pl.when(col == 3)(lambda: zero_i(NI + 1))

    def remote(src, dst, s, n, device):
        return pltpu.make_async_remote_copy(src, dst, s_sem.at[s, n], r_sem.at[s, n], device_id=device, device_id_type=MESH)

    def j_copy(s, way, g):
        start, n = GROUPS[g]
        rows = pl.ds(start + 1, n)
        a, b = (NJ, 0) if way == UP else (1, NJ + 1)
        return remote(u[s].at[a, rows, CELLS], u[s].at[b, rows, CELLS], s, way + g, to[way])

    def i_copy(s, way):
        a, b = (NI, 0) if way == I_UP else (1, NI + 1)
        return remote(u[s].at[pl.ds(1, NJ), a, CELLS], u[s].at[pl.ds(1, NJ), b, CELLS], s, way, to[way])

    def k_copy(s, g):
        start, n = GROUPS[g]
        rows = pl.ds(start, n)
        return remote(kf.at[s, rows], kh.at[s, rows], s, KF + g, {"slabs": 1 - slab})

    def take_k(s, groups):
        def body(i):
            for j in range(NJ):
                kf[s, i, pl.ds(j, 1), :] = u[s][j + 1, i + 1, pl.ds(face_row, 1), :]

        rows_of(groups, body)

    def put_k(s, groups):
        def body(i):
            for j in range(NJ):
                u[s][j + 1, i + 1, pl.ds(halo_row, 1), :] = kh[s, i, pl.ds(j, 1), :]

        rows_of(groups, body)

    def each_j(s, gs, act):
        for g in gs:
            for way in (UP, DOWN):

                @pl.when(has[way])
                def _(way=way, g=g):
                    act(j_copy(s, way, g))

    def send_i(s):
        for way in (I_UP, I_DOWN):

            @pl.when(has[way])
            def _(way=way):
                i_copy(s, way).start()

    def send_k(s, gs):
        for g in gs:
            k_copy(s, g).start()

    def recv_i(s):
        for way, back in ((I_UP, I_DOWN), (I_DOWN, I_UP)):

            @pl.when(has[back])
            def _(way=way):
                i_copy(s, way).wait_recv()

    def recv_j(s, gs):
        for g in gs:
            for way, back in ((UP, DOWN), (DOWN, UP)):

                @pl.when(has[back])
                def _(way=way, g=g):
                    j_copy(s, way, g).wait_recv()

    def recv_k(s, gs):
        for g in gs:
            k_copy(s, g).wait_recv()

    def march(s, groups):
        b = u[s]

        def body(i):
            for k in range(0, NK, 8):
                here, lower, upper = pl.ds(K0 + k, 8), pl.ds(K0 + k - 1, 8), pl.ds(K0 + k + 1, 8)
                prev, mid = b[0, i + 1, here, :], b[1, i + 1, here, :]
                for j in range(1, NJ + 1):
                    following = b[j + 1, i + 1, here, :]
                    near = (prev + following) + (b[j, i, here, :] + b[j, i + 2, here, :])
                    near = near + (b[j, i + 1, lower, :] + b[j, i + 1, upper, :])
                    new = mid * (0.6 - 0.2 * (mid * c[j - 1, i, pl.ds(k, 8), :])) + 0.1 * near
                    if s + 1 < STEPS:
                        u[s + 1][j, i + 1, here, :] = new
                    else:
                        out[j - 1, i, pl.ds(k, 8), :] = new
                    prev, mid = mid, following

        rows_of(groups, body)

    first = jnp.where(r == 0, 0.1, 0.0).astype(F32)
    later = jnp.where(r == 0, 0.0, 0.1).astype(F32)

    def block_totals(groups):
        b = u[2]

        def body(i):
            for k in range(0, NK, 8):
                here, lower, upper = pl.ds(K0 + k, 8), pl.ds(K0 + k - 1, 8), pl.ds(K0 + k + 1, 8)
                own, near = None, None
                for j in range(1, NJ + 1):
                    mid = b[j, i + 1, here, :]
                    term = mid * (0.8 - 0.2 * (mid * c[j - 1, i, pl.ds(k, 8), :]))
                    if j == 1:
                        term = term - first * mid
                    beside = (b[j, i, here, :] + b[j, i + 2, here, :]) + (b[j, i + 1, lower, :] + b[j, i + 1, upper, :])
                    own = term if own is None else own + term
                    near = beside if near is None else near + beside
                tot[i, pl.ds(k, 8), :] = own + 0.1 * near

        rows_of(groups, body)

    def p_copy(n, src, dst, device):
        return pltpu.make_async_remote_copy(src, dst, ps_sem.at[n], pr_sem.at[n], device_id=device, device_id_type=MESH)

    parts = ((4 + 4 * core, 4), (1 + 11 * core, 3), (15 * core, 1))
    parts_p = ((8 - 4 * core, 4), (12 - 11 * core, 3), (15 - 15 * core, 1))

    def t_copy(n):
        rows = (pl.ds(1, 14), pl.ds(0, 1), pl.ds(15, 1))[n]
        return p_copy(n, tot.at[rows], tot_p.at[rows], other_core)

    def y_copy(n):
        rows = pl.ds(*parts[n])
        return p_copy(3 + n, x_out.at[rows], x_in.at[rows], {"rows": r + 4})

    def x_copy(n, src):
        rows = pl.ds(*parts[n])
        return p_copy(6 + n, src.at[rows], p_in.at[rows], other_chip)

    def z_copy(n, mine=True):
        rows = pl.ds(*(parts if mine else parts_p)[n])
        return p_copy(9 + n, z.at[rows], z_p.at[rows], other_core)

    sends_x = ((x_lo == 0), (x_lo == 1) & (y > 0))
    takes_x = (x_lo == 1) | (y > 0)

    def chain(n):
        start, rows = parts[n]
        own = ((start, rows),)

        @pl.when(y > 0)
        def _():
            y_copy(n).wait_recv()

            def body(i):
                x_out[i] = x_in[i] + (tot[i] + tot_p[i])

            rows_of(own, body)

        @pl.when(y == 0)
        def _():
            def body(i):
                x_out[i] = tot[i] + tot_p[i]

            rows_of(own, body)

        pl.when(y < 3)(lambda: y_copy(n).start())
        pl.when(sends_x[0])(lambda: x_copy(n, x_out).start())
        pl.when(sends_x[1])(lambda: x_copy(n, x_in).start())

    def combine(n):
        own = (parts[n],)

        @pl.when(takes_x)
        def _():
            x_copy(n, x_out).wait_recv()

        @pl.when(y > 0)
        def _():
            def body(i):
                z[i] = x_in[i] + p_in[i]

            rows_of(own, body)

        @pl.when((y == 0) & (x_lo == 1))
        def _():
            def body(i):
                z[i] = p_in[i]

            rows_of(own, body)

        @pl.when((y == 0) & (x_lo == 0))
        def _():
            def body(i):
                z[i] = zero_plane

            rows_of(own, body)

        z_copy(n).start()

    pl.semaphore_wait(barrier, count)
    load_u.wait()
    send_i(0)
    take_k(0, ((0, NI),))
    send_k(0, (0, 1, 2))
    each_j(0, (0, 1, 2), lambda copy: copy.start())
    load_c.wait()

    for s in range(STEPS):
        if s == 2:
            recv_k(2, (0, 1, 2))
            put_k(2, ((0, NI),))
            block_totals(((1, 14),))
            t_copy(0).start()
            t_copy(0).wait_recv()
            chain(0)
            chain(1)
            recv_i(2)
            block_totals(((0, 1), (15, 1)))
            t_copy(1).start()
            t_copy(2).start()
            t_copy(1).wait_recv()
            t_copy(2).wait_recv()
            chain(2)
        else:
            recv_k(s, (0, 1))
            put_k(s, EDGE)
            recv_i(s)
        recv_j(s, (0, 1))
        march(s, EDGE)
        if s < 2:
            send_i(s + 1)
            take_k(s + 1, EDGE)
            send_k(s + 1, (0, 1))
            each_j(s + 1, (0, 1), lambda copy: copy.start())
            recv_k(s, (2,))
            put_k(s, MID)
        recv_j(s, (2,))
        march(s, MID)
        if s < 2:
            take_k(s + 1, MID)
            send_k(s + 1, (2,))
            each_j(s + 1, (2,), lambda copy: copy.start())

    for n in range(3):
        combine(n)

    def finish(groups, get):
        def body(i):
            below[i] = get(i) + later * (u2[1, i + 1, CELLS, :] - u2[0, i + 1, CELLS, :])

        rows_of(groups, body)

    def finish_part(part, src):
        pl.when(core == 0)(lambda: finish((part,), lambda i: src[i]))
        pl.when(core == 1)(lambda: finish((part,), lambda i: src[i] + tot_p[i]))

    for n in range(3):
        finish_part(parts[n], z)
    for n in range(3):
        z_copy(n, mine=False).wait_recv()
        finish_part(parts_p[n], z_p)

    for s in range(STEPS):
        each_j(s, (0, 1, 2), lambda copy: copy.wait_send())
        for way in (I_UP, I_DOWN):

            @pl.when(has[way])
            def _(way=way, s=s):
                i_copy(s, way).wait_send()

        for g in range(3):
            k_copy(s, g).wait_send()
    for n in range(3):
        t_copy(n).wait_send()
        z_copy(n).wait_send()
        pl.when(y < 3)(lambda n=n: y_copy(n).wait_send())
        pl.when(sends_x[0] | sends_x[1])(lambda n=n: x_copy(n, x_out).wait_send())


def write_kernel(v, below, pot, end, pot_v, sem):
    copies = [pltpu.make_async_copy(v, end, sem.at[0])]
    copies[0].start()
    for q in range(4):

        def body(i, _):
            for k in range(0, NK, 8):
                here = pl.ds(k, 8)
                total = below[i, here, :]
                for j in range(NJ):
                    total = total + v[j, i, here, :]
                    pot_v[j, i, here, :] = total * (1.0 / 128.0)
            return 0

        lax.fori_loop(4 * q, 4 * q + 4, body, 0)
        rows = pl.ds(4 * q, 4)
        copy = pltpu.make_async_copy(pot_v.at[:, rows], pot.at[:, rows], sem.at[1 + q])
        copy.start()
        copies.append(copy)
    for copy in copies:
        copy.wait()


def on_device(field_values, crowding):
    block = (NJ, NI, NK, NL)
    plane = (NI, NK, NL)
    padded = (NJ + 2, NI + 2, NK + 16, NL)
    vmem = pl.BlockSpec(memory_space=pltpu.VMEM)
    hbm = pl.BlockSpec(memory_space=pltpu.HBM)
    sems = pltpu.SemaphoreType.DMA
    out, below = pl.pallas_call(
        exchange_kernel,
        out_shape=(pltpu.VMEM(block, F32), pltpu.VMEM(plane, F32)),
        in_specs=[hbm, hbm],
        out_specs=(vmem, vmem),
        scratch_shapes=[pltpu.VMEM(padded, F32)] * 3
        + [pltpu.VMEM(block, F32)]
        + [pltpu.VMEM((STEPS, NI, NJ, NL), F32)] * 2
        + [pltpu.VMEM(plane, F32)] * 7
        + [sems((2,)), sems((STEPS, N_SEM)), sems((STEPS, N_SEM)), sems((12,)), sems((12,))],
        compiler_params=pltpu.CompilerParams(collective_id=1, has_side_effects=True, vmem_limit_bytes=44 * 2**20),
        name="exchange",
    )(field_values, crowding)
    full = jax.ShapeDtypeStruct(block, F32)
    return pl.pallas_call(
        write_kernel,
        out_shape=(full, full),
        in_specs=[vmem, vmem],
        out_specs=(hbm, hbm),
        scratch_shapes=[pltpu.VMEM(block, F32), sems((5,))],
        compiler_params=pltpu.CompilerParams(vmem_limit_bytes=16 * 2**20),
        name="write",
    )(out, below)


def solution(mesh):
    spec = P(("trial", "rows"), "cols", "slabs", None)
    return jax.shard_map(on_device, mesh=mesh, in_specs=(spec, spec), out_specs=(spec, spec), check_vma=False)
```

```python
import functools

import jax
import jax.numpy as jnp
from jax import lax
from jax.experimental import pallas as pl
from jax.experimental.pallas import tpu as pltpu
from jax.sharding import PartitionSpec as P

MESH = pl.DeviceIdType.MESH
F32 = jnp.float32
STEPS = 3
NJ, NI, NK, NL = 8, 16, 64, 128
K0 = 8
EDGE = ((0, 4), (12, 4))
MID = ((4, 8),)
GROUPS = EDGE + MID
CELLS = pl.ds(K0, NK)
N_SEM = 15
UP, DOWN, I_UP, I_DOWN, KF, RELAY, FORWARD = 0, 3, 6, 8, 10, 13, 14


CHUNKS = 6


def rows_of(groups, body):
    for start, count in groups:
        lax.fori_loop(start, start + count, lambda i, _: (body(i), 0)[1], 0)


def exchange_kernel(fv, cr, out, below, u0, u1, u2, c, kf, kh, held, tot, tot_p, x_in, x_out, p_in, z, z_p, load_sem, s_sem, r_sem, ps_sem, pr_sem):
    r, col, slab = lax.axis_index("rows"), lax.axis_index("cols"), lax.axis_index("slabs")
    core = lax.rem(r, 2)
    x_lo = lax.rem(lax.div(r, 2), 2)
    y = lax.div(r, 4)
    u = (u0, u1, u2)
    other_core = {"rows": r + 1 - 2 * core}
    other_chip = {"rows": r + 2 - 4 * x_lo}
    via = {"rows": r + 2 - 4 * x_lo, "cols": col + 1 - 2 * lax.rem(col, 2)}
    onward = {"rows": r + 2 - 4 * x_lo, "cols": lax.rem(col + 2, 4)}

    has = {UP: r < 15, DOWN: r > 0, I_UP: col < 3, I_DOWN: col > 0}
    to = {UP: {"rows": r + 1}, DOWN: {"rows": r - 1}, I_UP: {"cols": col + 1}, I_DOWN: {"cols": col - 1}}
    barrier = pltpu.get_barrier_semaphore()
    count = jnp.int32(4)
    for way in (UP, DOWN, I_UP, I_DOWN):
        count = count + jnp.where(has[way], 1, 0)

        @pl.when(has[way])
        def _(way=way):
            pl.semaphore_signal(barrier, 1, device_id=to[way], device_id_type=MESH)

    for ok, dst in ((y < 3, {"rows": r + 4}), (y > 0, {"rows": r - 4})):
        count = count + jnp.where(ok, 1, 0)

        @pl.when(ok)
        def _(dst=dst):
            pl.semaphore_signal(barrier, 1, device_id=dst, device_id_type=MESH)

    pl.semaphore_signal(barrier, 1, device_id={"slabs": 1 - slab}, device_id_type=MESH)
    for dst in (other_chip, via, onward):
        pl.semaphore_signal(barrier, 1, device_id=dst, device_id_type=MESH)

    load_u = pltpu.make_async_copy(fv, u0.at[pl.ds(1, NJ), pl.ds(1, NI), CELLS], load_sem.at[0])
    load_c = pltpu.make_async_copy(cr, c, load_sem.at[1])
    load_u.start()
    load_c.start()

    edge_row = jnp.where(slab == 0, K0 - 1, K0 + NK)
    halo_row = jnp.where(slab == 0, K0 + NK, K0 - 1)
    face_row = jnp.where(slab == 0, K0 + NK - 1, K0)
    zero_plane = jnp.zeros((NK, NL), F32)
    zero_line = jnp.zeros((1, NL), F32)

    def zero_lines(i):
        for b in u:
            for j in range(NJ):
                b[j + 1, i + 1, pl.ds(edge_row, 1), :] = zero_line

    rows_of(((0, NI),), zero_lines)

    def zero_j(plane):
        def body(i):
            for b in u:
                b[plane, i + 1, CELLS, :] = zero_plane

        rows_of(((0, NI),), body)

    def zero_i(row):
        def body(j):
            for b in u:
                b[j + 1, row, CELLS, :] = zero_plane

        rows_of(((0, NJ),), body)

    pl.when(r == 0)(lambda: zero_j(0))
    pl.when(r == 15)(lambda: zero_j(NJ + 1))
    pl.when(col == 0)(lambda: zero_i(0))
    pl.when(col == 3)(lambda: zero_i(NI + 1))

    def remote(src, dst, s, n, device, n_recv=None):
        recv = r_sem.at[s, n if n_recv is None else n_recv]
        return pltpu.make_async_remote_copy(src, dst, s_sem.at[s, n], recv, device_id=device, device_id_type=MESH)

    def j_copy(s, way, g):
        start, n = GROUPS[g]
        rows = pl.ds(start + 1, n)
        a, b = (NJ, 0) if way == UP else (1, NJ + 1)
        return remote(u[s].at[a, rows, CELLS], u[s].at[b, rows, CELLS], s, way + g, to[way])

    def i_ref(s, half, row):
        return u[s].at[pl.ds(1 + 4 * half, 4), row, CELLS]

    def i_copy(s, way, half):
        a, b = (NI, 0) if way == I_UP else (1, NI + 1)
        return remote(i_ref(s, half, a), i_ref(s, half, b), s, way + half, to[way])

    def relay_copy(s, way):
        return remote(i_ref(s, 1, NI if way == I_UP else 1), held.at[s], s, RELAY, via)

    def forward_copy(s, way):
        return remote(held.at[s], i_ref(s, 1, 0 if way == I_UP else NI + 1), s, FORWARD, onward, way + 1)

    relayed = {I_UP: col == 1, I_DOWN: col == 2}
    forwards = {I_UP: col == 0, I_DOWN: col == 3}
    direct = {I_UP: (col == 0) | (col == 2), I_DOWN: (col == 1) | (col == 3)}

    def each_i(s, act):
        for way in (I_UP, I_DOWN):
            pl.when(relayed[way])(lambda way=way: act(relay_copy(s, way)))
        for way in (I_UP, I_DOWN):
            pl.when(has[way])(lambda way=way: act(i_copy(s, way, 0)))
            pl.when(direct[way])(lambda way=way: act(i_copy(s, way, 1)))

    def forward(s):
        for way in (I_UP, I_DOWN):

            @pl.when(forwards[way])
            def _(way=way):
                relay_copy(s, way).wait_recv()
                forward_copy(s, way).start()

    def k_copy(s, g):
        start, n = GROUPS[g]
        rows = pl.ds(start, n)
        return remote(kf.at[s, rows], kh.at[s, rows], s, KF + g, {"slabs": 1 - slab})

    def take_k(s, groups):
        def body(i):
            for j in range(NJ):
                kf[s, i, pl.ds(j, 1), :] = u[s][j + 1, i + 1, pl.ds(face_row, 1), :]

        rows_of(groups, body)

    def put_k(s, groups):
        def body(i):
            for j in range(NJ):
                u[s][j + 1, i + 1, pl.ds(halo_row, 1), :] = kh[s, i, pl.ds(j, 1), :]

        rows_of(groups, body)

    def each_j(s, gs, act):
        for g in gs:
            for way in (UP, DOWN):

                @pl.when(has[way])
                def _(way=way, g=g):
                    act(j_copy(s, way, g))

    def send_i(s):
        each_i(s, lambda copy: copy.start())

    def send_k(s, gs):
        for g in gs:
            k_copy(s, g).start()

    def recv_i(s):
        for way, back in ((I_UP, I_DOWN), (I_DOWN, I_UP)):

            @pl.when(has[back])
            def _(way=way):
                i_copy(s, way, 0).wait_recv()
                i_copy(s, way, 1).wait_recv()

    def recv_j(s, gs):
        for g in gs:
            for way, back in ((UP, DOWN), (DOWN, UP)):

                @pl.when(has[back])
                def _(way=way, g=g):
                    j_copy(s, way, g).wait_recv()

    def recv_k(s, gs):
        for g in gs:
            k_copy(s, g).wait_recv()

    def march(s, groups):
        b = u[s]

        def body(i):
            for k in range(0, NK, 8):
                here, lower, upper = pl.ds(K0 + k, 8), pl.ds(K0 + k - 1, 8), pl.ds(K0 + k + 1, 8)
                prev, mid = b[0, i + 1, here, :], b[1, i + 1, here, :]
                for j in range(1, NJ + 1):
                    following = b[j + 1, i + 1, here, :]
                    near = (prev + following) + (b[j, i, here, :] + b[j, i + 2, here, :])
                    near = near + (b[j, i + 1, lower, :] + b[j, i + 1, upper, :])
                    new = mid * (0.6 - 0.2 * (mid * c[j - 1, i, pl.ds(k, 8), :])) + 0.1 * near
                    if s + 1 < STEPS:
                        u[s + 1][j, i + 1, here, :] = new
                    else:
                        out[j - 1, i, pl.ds(k, 8), :] = new
                    prev, mid = mid, following

        rows_of(groups, body)

    first = jnp.where(r == 0, 0.1, 0.0).astype(F32)
    later = jnp.where(r == 0, 0.0, 0.1).astype(F32)

    k_main = pl.multiple_of(8 * slab, 8)
    k_edge = pl.multiple_of(NK - 8 - (NK - 8) * slab, 8)

    def block_totals(groups, tiles):
        b = u[2]

        def body(i):
            for k in tiles:
                here, lower, upper = pl.ds(K0 + k, 8), pl.ds(K0 + k - 1, 8), pl.ds(K0 + k + 1, 8)
                own, near = None, None
                for j in range(1, NJ + 1):
                    mid = b[j, i + 1, here, :]
                    term = mid * (0.8 - 0.2 * (mid * c[j - 1, i, pl.ds(k, 8), :]))
                    if j == 1:
                        term = term - first * mid
                    beside = (b[j, i, here, :] + b[j, i + 2, here, :]) + (b[j, i + 1, lower, :] + b[j, i + 1, upper, :])
                    own = term if own is None else own + term
                    near = beside if near is None else near + beside
                tot[i, pl.ds(k, 8), :] = own + 0.1 * near

        rows_of(groups, body)

    def p_copy(n, src, dst, device):
        return pltpu.make_async_remote_copy(src, dst, ps_sem.at[n], pr_sem.at[n], device_id=device, device_id_type=MESH)

    all_k, main, edge = pl.ds(0, NK), pl.ds(k_main, NK - 8), pl.ds(k_edge, 8)
    main_tiles = [pl.multiple_of(k_main + 8 * t, 8) for t in range(NK // 8 - 1)]
    pieces = ((1, 13, 2, main), (3, 11, 2, main), (5, 9, 2, main), (7, 8, 1, main), (1, 8, 7, edge), (0, 15, 1, all_k))
    parts = [(a + (b - a) * core, n, k) for a, b, n, k in pieces]
    parts_p = [(b + (a - b) * core, n, k) for a, b, n, k in pieces]

    def at(ref, part):
        start, n, k = part
        return ref.at[pl.ds(start, n), k]

    def t_copy(n):
        part = ((1, 2, main), (13, 2, main), (3, 10, main), (1, 14, edge), (0, 1, all_k), (15, 1, all_k))[n]
        return p_copy(n, at(tot, part), at(tot_p, part), other_core)

    def y_copy(n):
        return p_copy(6 + n, at(x_out, parts[n]), at(x_in, parts[n]), {"rows": r + 4})

    def x_copy(n, src):
        return p_copy(6 + CHUNKS + n, at(src, parts[n]), at(p_in, parts[n]), other_chip)

    def z_copy(n, mine=True):
        part = (parts if mine else parts_p)[n]
        return p_copy(6 + 2 * CHUNKS + n, at(z, part), at(z_p, part), other_core)

    def over(part, body):
        start, n, k = part
        rows_of(((start, n),), lambda i: body(i, k))

    sends_x = ((x_lo == 0), (x_lo == 1) & (y > 0))
    takes_x = (x_lo == 1) | (y > 0)

    def chain(n):
        @pl.when(y > 0)
        def _():
            y_copy(n).wait_recv()

            def body(i, k):
                x_out[i, k, :] = x_in[i, k, :] + (tot[i, k, :] + tot_p[i, k, :])

            over(parts[n], body)

        @pl.when(y == 0)
        def _():
            def body(i, k):
                x_out[i, k, :] = tot[i, k, :] + tot_p[i, k, :]

            over(parts[n], body)

        pl.when(y < 3)(lambda: y_copy(n).start())
        pl.when(sends_x[0])(lambda: x_copy(n, x_out).start())
        pl.when(sends_x[1])(lambda: x_copy(n, x_in).start())

    def combine(n):
        @pl.when(takes_x)
        def _():
            x_copy(n, x_out).wait_recv()

        @pl.when(y > 0)
        def _():
            def body(i, k):
                z[i, k, :] = x_in[i, k, :] + p_in[i, k, :]

            over(parts[n], body)

        @pl.when((y == 0) & (x_lo == 1))
        def _():
            def body(i, k):
                z[i, k, :] = p_in[i, k, :]

            over(parts[n], body)

        @pl.when((y == 0) & (x_lo == 0))
        def _():
            def body(i, k):
                z[i, k, :] = jnp.zeros((8 if n == 4 else NK if n == 5 else NK - 8, NL), F32)

            over(parts[n], body)

        z_copy(n).start()

    pl.semaphore_wait(barrier, count)
    load_u.wait()
    send_i(0)
    take_k(0, ((0, NI),))
    send_k(0, (0, 1, 2))
    each_j(0, (0, 1, 2), lambda copy: copy.start())
    forward(0)
    load_c.wait()

    for s in range(STEPS):
        if s == 2:
            block_totals(((3, 10),), main_tiles)
            t_copy(2).start()
            pl.when(y > 0)(lambda: chain(0))
            t_copy(2).wait_recv()
            for n in (1, 2, 3):
                chain(n)
            recv_k(2, (0, 1, 2))
            put_k(2, ((0, NI),))
            recv_i(2)
            block_totals(((1, 14),), [k_edge])
            block_totals(((0, 1), (15, 1)), range(0, NK, 8))
            for n in (3, 4, 5):
                t_copy(n).start()
            for n in (3, 4, 5):
                t_copy(n).wait_recv()
            chain(4)
            chain(5)
        else:
            recv_k(s, (0, 1))
            put_k(s, EDGE)
            recv_i(s)
        recv_j(s, (0, 1))
        march(s, EDGE)
        if s < 2:
            send_i(s + 1)
            take_k(s + 1, EDGE)
            send_k(s + 1, (0, 1))
            each_j(s + 1, (0, 1), lambda copy: copy.start())
            forward(s + 1)
            if s == 1:
                block_totals(((1, 2), (13, 2)), main_tiles)
                t_copy(0).start()
                t_copy(1).start()
                t_copy(0).wait_recv()
                t_copy(1).wait_recv()
                pl.when(y == 0)(lambda: chain(0))
            recv_k(s, (2,))
            put_k(s, MID)
        recv_j(s, (2,))
        march(s, MID)
        if s < 2:
            take_k(s + 1, MID)
            send_k(s + 1, (2,))
            each_j(s + 1, (2,), lambda copy: copy.start())

    for n in range(CHUNKS):
        combine(n)

    def finish(part, src):
        def body(i, k):
            cells = pl.ds(pl.multiple_of(K0 + k.start, 8), k.size)
            extra = later * (u2[1, i + 1, cells, :] - u2[0, i + 1, cells, :])
            below[i, k, :] = src[i, k, :] + (extra + jnp.where(core == 1, tot_p[i, k, :], 0.0))

        over(part, body)

    for n in range(CHUNKS):
        finish(parts[n], z)
    for n in range(CHUNKS):
        z_copy(n, mine=False).wait_recv()
        finish(parts_p[n], z_p)

    for s in range(STEPS):
        each_j(s, (0, 1, 2), lambda copy: copy.wait_send())
        each_i(s, lambda copy: copy.wait_send())
        for way in (I_UP, I_DOWN):
            pl.when(forwards[way])(lambda way=way, s=s: forward_copy(s, way).wait_send())
        for g in range(3):
            k_copy(s, g).wait_send()
    for n in range(6):
        t_copy(n).wait_send()
    for n in range(CHUNKS):
        z_copy(n).wait_send()
        pl.when(y < 3)(lambda n=n: y_copy(n).wait_send())
        pl.when(sends_x[0] | sends_x[1])(lambda n=n: x_copy(n, x_out).wait_send())


def write_kernel(v, below, pot, end, pot_v, sem):
    copies = [pltpu.make_async_copy(v, end, sem.at[0])]
    copies[0].start()
    for q in range(4):

        def body(i, _):
            for k in range(0, NK, 8):
                here = pl.ds(k, 8)
                total = below[i, here, :]
                for j in range(NJ):
                    total = total + v[j, i, here, :]
                    pot_v[j, i, here, :] = total * (1.0 / 128.0)
            return 0

        lax.fori_loop(4 * q, 4 * q + 4, body, 0)
        rows = pl.ds(4 * q, 4)
        copy = pltpu.make_async_copy(pot_v.at[:, rows], pot.at[:, rows], sem.at[1 + q])
        copy.start()
        copies.append(copy)
    for copy in copies:
        copy.wait()


def on_device(field_values, crowding):
    block = (NJ, NI, NK, NL)
    plane = (NI, NK, NL)
    padded = (NJ + 2, NI + 2, NK + 16, NL)
    vmem = pl.BlockSpec(memory_space=pltpu.VMEM)
    hbm = pl.BlockSpec(memory_space=pltpu.HBM)
    sems = pltpu.SemaphoreType.DMA
    out, below = pl.pallas_call(
        exchange_kernel,
        out_shape=(pltpu.VMEM(block, F32), pltpu.VMEM(plane, F32)),
        in_specs=[hbm, hbm],
        out_specs=(vmem, vmem),
        scratch_shapes=[pltpu.VMEM(padded, F32)] * 3
        + [pltpu.VMEM(block, F32)]
        + [pltpu.VMEM((STEPS, NI, NJ, NL), F32)] * 2
        + [pltpu.VMEM((STEPS, 4, NK, NL), F32)]
        + [pltpu.VMEM(plane, F32)] * 7
        + [sems((2,)), sems((STEPS, N_SEM)), sems((STEPS, N_SEM)), sems((6 + 3 * CHUNKS,)), sems((6 + 3 * CHUNKS,))],
        compiler_params=pltpu.CompilerParams(collective_id=1, has_side_effects=True, vmem_limit_bytes=57 * 2**20),
        name="exchange",
    )(field_values, crowding)
    full = jax.ShapeDtypeStruct(block, F32)
    return pl.pallas_call(
        write_kernel,
        out_shape=(full, full),
        in_specs=[vmem, vmem],
        out_specs=(hbm, hbm),
        scratch_shapes=[pltpu.VMEM(block, F32), sems((5,))],
        compiler_params=pltpu.CompilerParams(vmem_limit_bytes=16 * 2**20),
        name="write",
    )(out, below)


def solution(mesh):
    spec = P(("trial", "rows"), "cols", "slabs", None)
    return jax.shard_map(on_device, mesh=mesh, in_specs=(spec, spec), out_specs=(spec, spec), check_vma=False)
```

```python
import functools

import jax
import jax.numpy as jnp
from jax import lax
from jax.experimental import pallas as pl
from jax.experimental.pallas import tpu as pltpu
from jax.sharding import PartitionSpec as P

MESH = pl.DeviceIdType.MESH
F32 = jnp.float32
STEPS = 3
NJ, NI, NK, NL = 8, 16, 64, 128
K0 = 8
PIECES = ((0, 1), (15, 1), (1, 4), (11, 4), (5, 4), (9, 2))
WAVES = ((0, 1), (2, 3), (4, 5))
DETOUR = (2, 4, 3)
CELLS = pl.ds(K0, NK)
N_SEM = 30
UP, DOWN, I_UP, I_DOWN, KF, RELAY, FORWARD, J_RELAY, J_FORWARD = 0, 6, 12, 14, 16, 22, 23, 24, 27

CHUNKS = 5


def rows_of(groups, body):
    for start, count in groups:
        lax.fori_loop(start, start + count, lambda i, _: (body(i), 0)[1], 0)


def exchange_kernel(fv, cr, out, below, u0, u1, u2, c, kf, kh, held, held_j, tot, tot_p, x_in, x_out, p_in, z, z_p, load_sem, go_sem, s_sem, r_sem, ps_sem, pr_sem):
    r, col, slab = lax.axis_index("rows"), lax.axis_index("cols"), lax.axis_index("slabs")
    core = lax.rem(r, 2)
    x_lo = lax.rem(lax.div(r, 2), 2)
    y = lax.div(r, 4)
    u = (u0, u1, u2)
    other_core = {"rows": r + 1 - 2 * core}
    other_chip = {"rows": r + 2 - 4 * x_lo}
    via = {"rows": r + 2 - 4 * x_lo, "cols": col + 1 - 2 * lax.rem(col, 2)}
    onward = {"rows": r + 2 - 4 * x_lo, "cols": lax.rem(col + 2, 4)}

    has = {UP: r < 15, DOWN: r > 0, I_UP: col < 3, I_DOWN: col > 0}
    to = {UP: {"rows": r + 1}, DOWN: {"rows": r - 1}, I_UP: {"cols": col + 1}, I_DOWN: {"cols": col - 1}}
    top, bottom = lax.rem(r, 4) == 3, lax.rem(r, 4) == 0
    across = {"rows": jnp.where(top, r - 3, r + 3)}
    over_slab = {"slabs": 1 - slab}
    near_col = {"cols": col + 1 - 2 * lax.rem(col, 2)}
    yes = r >= 0
    greets = (
        (has[UP], to[UP], has[UP]),
        (has[DOWN], to[DOWN], has[DOWN]),
        (y < 3, {"rows": r + 4}, y < 3),
        (y > 0, {"rows": r - 4}, y > 0),
        (top | bottom, across, top | bottom),
        (yes, other_chip, yes),
        (yes, near_col, yes),
        (yes, via, yes),
        (slab == 0, over_slab, slab == 1),
        (col == 1, to[I_UP], col == 2),
        (col < 2, onward, col > 1),
    )
    barrier = pltpu.get_barrier_semaphore()
    count = jnp.int32(0)
    for signals, dst, signalled in greets:
        count = count + jnp.where(signalled, 1, 0)

        @pl.when(signals)
        def _(dst=dst):
            pl.semaphore_signal(barrier, 1, device_id=dst, device_id_type=MESH)

    load_u = pltpu.make_async_copy(fv, u0.at[pl.ds(1, NJ), pl.ds(1, NI), CELLS], load_sem.at[0])
    load_c = pltpu.make_async_copy(cr, c, load_sem.at[1])
    load_u.start()
    load_c.start()

    edge_row = jnp.where(slab == 0, K0 - 1, K0 + NK)
    halo_row = jnp.where(slab == 0, K0 + NK, K0 - 1)
    face_row = jnp.where(slab == 0, K0 + NK - 1, K0)
    zero_plane = jnp.zeros((NK, NL), F32)
    zero_line = jnp.zeros((1, NL), F32)

    def zero_lines(i):
        for b in u:
            for j in range(NJ):
                b[j + 1, i + 1, pl.ds(edge_row, 1), :] = zero_line

    rows_of(((0, NI),), zero_lines)

    def zero_j(plane):
        def body(i):
            for b in u:
                b[plane, i + 1, CELLS, :] = zero_plane

        rows_of(((0, NI),), body)

    def zero_i(row):
        def body(j):
            for b in u:
                b[j + 1, row, CELLS, :] = zero_plane

        rows_of(((0, NJ),), body)

    pl.when(r == 0)(lambda: zero_j(0))
    pl.when(r == 15)(lambda: zero_j(NJ + 1))
    pl.when(col == 0)(lambda: zero_i(0))
    pl.when(col == 3)(lambda: zero_i(NI + 1))

    def remote(src, dst, s, n, device, n_recv=None):
        recv = r_sem.at[s, n if n_recv is None else n_recv]
        return pltpu.make_async_remote_copy(src, dst, s_sem.at[s, n], recv, device_id=device, device_id_type=MESH)

    def j_ref(s, g, plane):
        start, n = PIECES[g]
        return u[s].at[plane, pl.ds(start + 1, n), CELLS]

    def j_copy(s, way, g):
        a, b = (NJ, 0) if way == UP else (1, NJ + 1)
        return remote(j_ref(s, g, a), j_ref(s, g, b), s, way + g, to[way])

    def j_relay(s, way, g):
        n = DETOUR.index(g)
        far = {"rows": r + 4 if way == UP else r - 4}
        return remote(j_ref(s, g, NJ if way == UP else 1), held_j.at[s, n], s, J_RELAY + n, far)

    def j_onward(s, way, g):
        n = DETOUR.index(g)
        return remote(held_j.at[s, n], j_ref(s, g, 0 if way == UP else NJ + 1), s, J_FORWARD + n, across, way + g)

    detours = {
        UP: {2: top & (y < 3), 4: top & (y < 3) & (y > 0), 3: top & (y == 2)},
        DOWN: {2: bottom & (y > 0), 4: bottom & (y > 0) & (y < 3), 3: bottom & (y == 1)},
    }
    passes = {
        UP: {2: top & (y > 0), 4: top & (y > 1), 3: top & (y == 3)},
        DOWN: {2: bottom & (y < 3), 4: bottom & (y < 2), 3: bottom & (y == 0)},
    }

    def i_ref(s, half, row):
        return u[s].at[pl.ds(1 + 4 * half, 4), row, CELLS]

    def i_copy(s, way, half):
        a, b = (NI, 0) if way == I_UP else (1, NI + 1)
        return remote(i_ref(s, half, a), i_ref(s, half, b), s, way + half, to[way])

    def relay_copy(s, way):
        return remote(i_ref(s, 1, NI if way == I_UP else 1), held.at[s], s, RELAY, via)

    def forward_copy(s, way):
        return remote(held.at[s], i_ref(s, 1, 0 if way == I_UP else NI + 1), s, FORWARD, onward, way + 1)

    relayed = {I_UP: col == 1, I_DOWN: col == 2}
    forwards = {I_UP: col == 0, I_DOWN: col == 3}
    direct = {I_UP: (col == 0) | (col == 2), I_DOWN: (col == 1) | (col == 3)}

    far = {I_UP: col == 1, I_DOWN: col == 2}

    def each_i(s, act, near=True, beyond=True):
        if near:
            for way in (I_UP, I_DOWN):
                pl.when(relayed[way])(lambda way=way: act(relay_copy(s, way)))
        for way in (I_UP, I_DOWN):
            if near:
                pl.when(direct[way])(lambda way=way: [act(i_copy(s, way, half)) for half in (0, 1)] and None)
            if beyond:
                pl.when(far[way])(lambda way=way: act(i_copy(s, way, 0)))

    def forward(s):
        for way in (I_UP, I_DOWN):

            @pl.when(forwards[way])
            def _(way=way):
                relay_copy(s, way).wait_recv()
                forward_copy(s, way).start()

    def k_copy(s, g):
        start, n = PIECES[g]
        rows = pl.ds(start, n)
        return remote(kf.at[s, rows], kh.at[s, rows], s, KF + g, {"slabs": 1 - slab})

    def take_k(s, groups):
        def body(i):
            for j in range(NJ):
                kf[s, i, pl.ds(j, 1), :] = u[s][j + 1, i + 1, pl.ds(face_row, 1), :]

        rows_of(groups, body)

    def put_k(s, groups):
        def body(i):
            for j in range(NJ):
                u[s][j + 1, i + 1, pl.ds(halo_row, 1), :] = kh[s, i, pl.ds(j, 1), :]

        rows_of(groups, body)

    def each_j(s, gs, act):
        for g in gs:
            for way in (UP, DOWN):
                straight = has[way]
                if g in DETOUR:
                    straight = straight & jnp.logical_not(detours[way][g])
                    pl.when(detours[way][g])(lambda way=way, g=g: act(j_relay(s, way, g)))
                pl.when(straight)(lambda way=way, g=g: act(j_copy(s, way, g)))

    def pass_j(s, gs):
        for g in gs:
            for way in (UP, DOWN):

                @pl.when(passes[way][g])
                def _(way=way, g=g):
                    j_relay(s, way, g).wait_recv()
                    j_onward(s, way, g).start()

    def send_i(s, **which):
        each_i(s, lambda copy: copy.start(), **which)

    def send_k(s, gs):
        for g in gs:
            k_copy(s, g).start()

    def recv_i(s):
        for way, back in ((I_UP, I_DOWN), (I_DOWN, I_UP)):

            @pl.when(has[back])
            def _(way=way):
                i_copy(s, way, 0).wait_recv()
                i_copy(s, way, 1).wait_recv()

    def recv_j(s, gs):
        for g in gs:
            for way, back in ((UP, DOWN), (DOWN, UP)):

                @pl.when(has[back])
                def _(way=way, g=g):
                    j_copy(s, way, g).wait_recv()

    def recv_k(s, gs):
        for g in gs:
            k_copy(s, g).wait_recv()

    def march(s, groups):
        b = u[s]

        def body(i):
            for k in range(0, NK, 8):
                here, lower, upper = pl.ds(K0 + k, 8), pl.ds(K0 + k - 1, 8), pl.ds(K0 + k + 1, 8)
                prev, mid = b[0, i + 1, here, :], b[1, i + 1, here, :]
                for j in range(1, NJ + 1):
                    following = b[j + 1, i + 1, here, :]
                    near = (prev + following) + (b[j, i, here, :] + b[j, i + 2, here, :])
                    near = near + (b[j, i + 1, lower, :] + b[j, i + 1, upper, :])
                    new = mid * (0.6 - 0.2 * (mid * c[j - 1, i, pl.ds(k, 8), :])) + 0.1 * near
                    if s + 1 < STEPS:
                        u[s + 1][j, i + 1, here, :] = new
                    else:
                        out[j - 1, i, pl.ds(k, 8), :] = new
                    prev, mid = mid, following

        rows_of(groups, body)

    first = jnp.where(r == 0, 0.1, 0.0).astype(F32)
    later = jnp.where(r == 0, 0.0, 0.1).astype(F32)

    k_main = pl.multiple_of(8 * slab, 8)
    k_edge = pl.multiple_of(NK - 8 - (NK - 8) * slab, 8)

    def block_totals(groups, tiles):
        b = u[2]

        def body(i):
            for k in tiles:
                here, lower, upper = pl.ds(K0 + k, 8), pl.ds(K0 + k - 1, 8), pl.ds(K0 + k + 1, 8)
                own, near = None, None
                for j in range(1, NJ + 1):
                    mid = b[j, i + 1, here, :]
                    term = mid * (0.8 - 0.2 * (mid * c[j - 1, i, pl.ds(k, 8), :]))
                    if j == 1:
                        term = term - first * mid
                    beside = (b[j, i, here, :] + b[j, i + 2, here, :]) + (b[j, i + 1, lower, :] + b[j, i + 1, upper, :])
                    own = term if own is None else own + term
                    near = beside if near is None else near + beside
                tot[i, pl.ds(k, 8), :] = own + 0.1 * near

        rows_of(groups, body)

    def p_copy(n, src, dst, device):
        return pltpu.make_async_remote_copy(src, dst, ps_sem.at[n], pr_sem.at[n], device_id=device, device_id_type=MESH)

    all_k, main, edge = pl.ds(0, NK), pl.ds(k_main, NK - 8), pl.ds(k_edge, 8)
    main_tiles = [pl.multiple_of(k_main + 8 * t, 8) for t in range(NK // 8 - 1)]
    pieces = ((1, 12, 3, main), (4, 10, 2, main), (6, 8, 2, main), (1, 8, 7, edge), (0, 15, 1, all_k))
    parts = [(a + (b - a) * core, n, k) for a, b, n, k in pieces]
    parts_p = [(b + (a - b) * core, n, k) for a, b, n, k in pieces]

    def at(ref, part):
        start, n, k = part
        return ref.at[pl.ds(start, n), k]

    def t_copy(n):
        part = ((1, 3, main), (12, 3, main), (4, 8, main), (1, 14, edge), (0, 1, all_k), (15, 1, all_k))[n]
        return p_copy(n, at(tot, part), at(tot_p, part), other_core)

    def y_copy(n):
        return p_copy(6 + n, at(x_out, parts[n]), at(x_in, parts[n]), {"rows": r + 4})

    def x_copy(n, src):
        return p_copy(6 + CHUNKS + n, at(src, parts[n]), at(p_in, parts[n]), other_chip)

    def z_copy(n, mine=True):
        part = (parts if mine else parts_p)[n]
        return p_copy(6 + 2 * CHUNKS + n, at(z, part), at(z_p, part), other_core)

    def over(part, body):
        start, n, k = part
        rows_of(((start, n),), lambda i: body(i, k))

    sends_x = ((x_lo == 0), (x_lo == 1) & (y > 0))
    takes_x = (x_lo == 1) | (y > 0)

    def chain(n):
        @pl.when(y > 0)
        def _():
            y_copy(n).wait_recv()

            def body(i, k):
                x_out[i, k, :] = x_in[i, k, :] + (tot[i, k, :] + tot_p[i, k, :])

            over(parts[n], body)

        @pl.when(y == 0)
        def _():
            def body(i, k):
                x_out[i, k, :] = tot[i, k, :] + tot_p[i, k, :]

            over(parts[n], body)

        pl.when(y < 3)(lambda: y_copy(n).start())
        pl.when(sends_x[0])(lambda: x_copy(n, x_out).start())
        pl.when(sends_x[1])(lambda: x_copy(n, x_in).start())

    def combine(n):
        @pl.when(takes_x)
        def _():
            x_copy(n, x_out).wait_recv()

        @pl.when(y > 0)
        def _():
            def body(i, k):
                z[i, k, :] = x_in[i, k, :] + p_in[i, k, :]

            over(parts[n], body)

        @pl.when((y == 0) & (x_lo == 1))
        def _():
            def body(i, k):
                z[i, k, :] = p_in[i, k, :]

            over(parts[n], body)

        @pl.when((y == 0) & (x_lo == 0))
        def _():
            def body(i, k):
                z[i, k, :] = jnp.zeros((8 if n == 3 else NK if n == 4 else NK - 8, NL), F32)

            over(parts[n], body)

        z_copy(n).start()

    pl.semaphore_wait(barrier, count)

    @pl.when(slab == 1)
    def _():
        pl.semaphore_signal(go_sem.at[0], 1, device_id=over_slab, device_id_type=MESH)

    @pl.when(col == 2)
    def _():
        pl.semaphore_signal(go_sem.at[1], 1, device_id=to[I_DOWN], device_id_type=MESH)
        pl.semaphore_signal(go_sem.at[1], 1, device_id=onward, device_id_type=MESH)

    load_u.wait()
    send_i(0, beyond=False)
    each_j(0, WAVES[0], lambda copy: copy.start())
    take_k(0, ((0, NI),))
    pl.when(col < 2)(lambda: pl.semaphore_wait(go_sem.at[1], 1))
    send_i(0, near=False)
    forward(0)
    pl.when(slab == 0)(lambda: pl.semaphore_wait(go_sem.at[0], 1))
    for wave in WAVES:
        send_k(0, wave)
    each_j(0, WAVES[1], lambda copy: copy.start())
    pass_j(0, (2, 3))
    each_j(0, WAVES[2], lambda copy: copy.start())
    pass_j(0, (4,))
    load_c.wait()

    for s in range(STEPS):
        if s == 2:
            block_totals(((4, 8),), main_tiles)
            t_copy(2).start()
            pl.when(y > 0)(lambda: chain(0))
            t_copy(2).wait_recv()
            pass_j(2, (4,))
            chain(1)
            chain(2)
            for wave in WAVES:
                recv_k(2, wave)
            put_k(2, PIECES)
            block_totals(((1, 14),), [k_edge])
            t_copy(3).start()
            t_copy(3).wait_recv()
            chain(3)
            recv_i(2)
            block_totals(((0, 1), (15, 1)), range(0, NK, 8))
            for n in (4, 5):
                t_copy(n).start()
            for n in (4, 5):
                t_copy(n).wait_recv()
            chain(4)
        for n, wave in enumerate(WAVES):
            rows = [PIECES[g] for g in wave]
            if s < 2:
                recv_k(s, wave)
                put_k(s, rows)
                if n == 0:
                    recv_i(s)
            recv_j(s, wave)
            if s == 1 and n == 0:
                pass_j(1, (4,))
            march(s, rows)
            if s < 2:
                if n == 0:
                    send_i(s + 1)
                take_k(s + 1, rows)
                send_k(s + 1, wave)
                each_j(s + 1, wave, lambda copy: copy.start())
                if n == 1:
                    forward(s + 1)
                    if s == 1:
                        block_totals(((1, 3), (12, 3)), main_tiles)
                        t_copy(0).start()
                        t_copy(1).start()
                    if s == 1:
                        t_copy(0).wait_recv()
                        t_copy(1).wait_recv()
                        pl.when(y == 0)(lambda: chain(0))
                elif n == 2:
                    pass_j(s + 1, (2, 3))

    for n in range(CHUNKS):
        combine(n)

    def finish(part, src):
        def body(i, k):
            cells = pl.ds(pl.multiple_of(K0 + k.start, 8), k.size)
            extra = later * (u2[1, i + 1, cells, :] - u2[0, i + 1, cells, :])
            below[i, k, :] = src[i, k, :] + (extra + jnp.where(core == 1, tot_p[i, k, :], 0.0))

        over(part, body)

    for n in range(CHUNKS):
        finish(parts[n], z)
    for n in range(CHUNKS):
        z_copy(n, mine=False).wait_recv()
        finish(parts_p[n], z_p)

    for s in range(STEPS):
        each_j(s, range(6), lambda copy: copy.wait_send())
        for g in DETOUR:
            for way in (UP, DOWN):
                pl.when(passes[way][g])(lambda way=way, g=g, s=s: j_onward(s, way, g).wait_send())
        each_i(s, lambda copy: copy.wait_send())
        for way in (I_UP, I_DOWN):
            pl.when(forwards[way])(lambda way=way, s=s: forward_copy(s, way).wait_send())
        for g in range(6):
            k_copy(s, g).wait_send()
    for n in range(6):
        t_copy(n).wait_send()
    for n in range(CHUNKS):
        z_copy(n).wait_send()
        pl.when(y < 3)(lambda n=n: y_copy(n).wait_send())
        pl.when(sends_x[0] | sends_x[1])(lambda n=n: x_copy(n, x_out).wait_send())


def write_kernel(v, below, pot, end, pot_v, sem):
    copies = [pltpu.make_async_copy(v, end, sem.at[0])]
    copies[0].start()
    for q in range(4):

        def body(i, _):
            for k in range(0, NK, 8):
                here = pl.ds(k, 8)
                total = below[i, here, :]
                for j in range(NJ):
                    total = total + v[j, i, here, :]
                    pot_v[j, i, here, :] = total * (1.0 / 128.0)
            return 0

        lax.fori_loop(4 * q, 4 * q + 4, body, 0)
        rows = pl.ds(4 * q, 4)
        copy = pltpu.make_async_copy(pot_v.at[:, rows], pot.at[:, rows], sem.at[1 + q])
        copy.start()
        copies.append(copy)
    for copy in copies:
        copy.wait()


def on_device(field_values, crowding):
    block = (NJ, NI, NK, NL)
    plane = (NI, NK, NL)
    padded = (NJ + 2, NI + 2, NK + 16, NL)
    vmem = pl.BlockSpec(memory_space=pltpu.VMEM)
    hbm = pl.BlockSpec(memory_space=pltpu.HBM)
    sems = pltpu.SemaphoreType.DMA
    out, below = pl.pallas_call(
        exchange_kernel,
        out_shape=(pltpu.VMEM(block, F32), pltpu.VMEM(plane, F32)),
        in_specs=[hbm, hbm],
        out_specs=(vmem, vmem),
        scratch_shapes=[pltpu.VMEM(padded, F32)] * 3
        + [pltpu.VMEM(block, F32)]
        + [pltpu.VMEM((STEPS, NI, NJ, NL), F32)] * 2
        + [pltpu.VMEM((STEPS, 4, NK, NL), F32), pltpu.VMEM((STEPS, len(DETOUR), 4, NK, NL), F32)]
        + [pltpu.VMEM(plane, F32)] * 7
        + [sems((2,)), pltpu.SemaphoreType.REGULAR((2,)), sems((STEPS, N_SEM)), sems((STEPS, N_SEM)), sems((6 + 3 * CHUNKS,)), sems((6 + 3 * CHUNKS,))],
        compiler_params=pltpu.CompilerParams(collective_id=1, has_side_effects=True, vmem_limit_bytes=57 * 2**20),
        name="exchange",
    )(field_values, crowding)
    full = jax.ShapeDtypeStruct(block, F32)
    return pl.pallas_call(
        write_kernel,
        out_shape=(full, full),
        in_specs=[vmem, vmem],
        out_specs=(hbm, hbm),
        scratch_shapes=[pltpu.VMEM(block, F32), sems((5,))],
        compiler_params=pltpu.CompilerParams(vmem_limit_bytes=16 * 2**20),
        name="write",
    )(out, below)


def solution(mesh):
    spec = P(("trial", "rows"), "cols", "slabs", None)
    return jax.shard_map(on_device, mesh=mesh, in_specs=(spec, spec), out_specs=(spec, spec), check_vma=False)
```

```python
import functools

import jax
import jax.numpy as jnp
from jax import lax
from jax.experimental import pallas as pl
from jax.experimental.pallas import tpu as pltpu
from jax.sharding import PartitionSpec as P

MESH = pl.DeviceIdType.MESH
F32 = jnp.float32
STEPS = 3
NJ, NI, NK, NL = 8, 16, 64, 128
K0 = 8
PIECES = ((0, 1), (15, 1), (1, 4), (11, 4), (5, 4), (9, 2))
WAVES = ((0, 1), (2, 3), (4, 5))
DETOUR = (2, 4, 3)
CELLS = pl.ds(K0, NK)
N_SEM = 30
UP, DOWN, I_UP, I_DOWN, KF, RELAY, FORWARD, J_RELAY, J_FORWARD = 0, 6, 12, 14, 16, 22, 23, 24, 27

CHUNKS = 5


def rows_of(groups, body):
    for start, count in groups:
        lax.fori_loop(start, start + count, lambda i, _: (body(i), 0)[1], 0)


def exchange_kernel(fv, cr, out, below, u0, u1, u2, c, kf, kh, held, held_j, tot, tot_p, x_in, x_out, p_in, z, z_p, chip, from_y, load_sem, go_sem, s_sem, r_sem, ps_sem, pr_sem):
    r, col, slab = lax.axis_index("rows"), lax.axis_index("cols"), lax.axis_index("slabs")
    core = lax.rem(r, 2)
    x_lo = lax.rem(lax.div(r, 2), 2)
    y = lax.div(r, 4)
    u = (u0, u1, u2)
    other_core = {"rows": r + 1 - 2 * core}
    other_chip = {"rows": r + 2 - 4 * x_lo}
    via = {"rows": r + 2 - 4 * x_lo, "cols": col + 1 - 2 * lax.rem(col, 2)}
    onward = {"rows": r + 2 - 4 * x_lo, "cols": lax.rem(col + 2, 4)}

    has = {UP: r < 15, DOWN: r > 0, I_UP: col < 3, I_DOWN: col > 0}
    to = {UP: {"rows": r + 1}, DOWN: {"rows": r - 1}, I_UP: {"cols": col + 1}, I_DOWN: {"cols": col - 1}}
    top, bottom = lax.rem(r, 4) == 3, lax.rem(r, 4) == 0
    across = {"rows": jnp.where(top, r - 3, r + 3)}
    over_slab = {"slabs": 1 - slab}
    near_col = {"cols": col + 1 - 2 * lax.rem(col, 2)}
    yes = r >= 0
    greets = (
        (has[UP], to[UP], has[UP]),
        (has[DOWN], to[DOWN], has[DOWN]),
        (y < 3, {"rows": r + 4}, y < 3),
        (y > 0, {"rows": r - 4}, y > 0),
        (y < 2, {"rows": r + 8}, y < 2),
        (y > 1, {"rows": r - 8}, y > 1),
        (y < 1, {"rows": r + 12}, y < 1),
        (y > 2, {"rows": r - 12}, y > 2),
        (top | bottom, across, top | bottom),
        (yes, other_chip, yes),
        (yes, near_col, yes),
        (yes, via, yes),
        (slab == 0, over_slab, slab == 1),
        (col == 1, to[I_UP], col == 2),
        (col < 2, onward, col > 1),
    )
    barrier = pltpu.get_barrier_semaphore()
    count = jnp.int32(0)
    for signals, dst, signalled in greets:
        count = count + jnp.where(signalled, 1, 0)

        @pl.when(signals)
        def _(dst=dst):
            pl.semaphore_signal(barrier, 1, device_id=dst, device_id_type=MESH)

    load_u = pltpu.make_async_copy(fv, u0.at[pl.ds(1, NJ), pl.ds(1, NI), CELLS], load_sem.at[0])
    load_c = pltpu.make_async_copy(cr, c, load_sem.at[1])
    load_u.start()
    load_c.start()

    edge_row = jnp.where(slab == 0, K0 - 1, K0 + NK)
    halo_row = jnp.where(slab == 0, K0 + NK, K0 - 1)
    face_row = jnp.where(slab == 0, K0 + NK - 1, K0)
    zero_plane = jnp.zeros((NK, NL), F32)
    zero_line = jnp.zeros((1, NL), F32)

    def zero_lines(i):
        for b in u:
            for j in range(NJ):
                b[j + 1, i + 1, pl.ds(edge_row, 1), :] = zero_line

    rows_of(((0, NI),), zero_lines)

    def zero_j(plane):
        def body(i):
            for b in u:
                b[plane, i + 1, CELLS, :] = zero_plane

        rows_of(((0, NI),), body)

    def zero_i(row):
        def body(j):
            for b in u:
                b[j + 1, row, CELLS, :] = zero_plane

        rows_of(((0, NJ),), body)

    pl.when(r == 0)(lambda: zero_j(0))
    pl.when(r == 15)(lambda: zero_j(NJ + 1))
    pl.when(col == 0)(lambda: zero_i(0))
    pl.when(col == 3)(lambda: zero_i(NI + 1))

    def remote(src, dst, s, n, device, n_recv=None):
        recv = r_sem.at[s, n if n_recv is None else n_recv]
        return pltpu.make_async_remote_copy(src, dst, s_sem.at[s, n], recv, device_id=device, device_id_type=MESH)

    def j_ref(s, g, plane):
        start, n = PIECES[g]
        return u[s].at[plane, pl.ds(start + 1, n), CELLS]

    def j_copy(s, way, g):
        a, b = (NJ, 0) if way == UP else (1, NJ + 1)
        return remote(j_ref(s, g, a), j_ref(s, g, b), s, way + g, to[way])

    def j_relay(s, way, g):
        n = DETOUR.index(g)
        far = {"rows": r + 4 if way == UP else r - 4}
        return remote(j_ref(s, g, NJ if way == UP else 1), held_j.at[s, n], s, J_RELAY + n, far)

    def j_onward(s, way, g):
        n = DETOUR.index(g)
        return remote(held_j.at[s, n], j_ref(s, g, 0 if way == UP else NJ + 1), s, J_FORWARD + n, across, way + g)

    detours = {
        UP: {2: top & (y < 3), 4: top & (y < 3) & (y > 0), 3: top & (y == 2)},
        DOWN: {2: bottom & (y > 0), 4: bottom & (y > 0) & (y < 3), 3: bottom & (y == 1)},
    }
    passes = {
        UP: {2: top & (y > 0), 4: top & (y > 1), 3: top & (y == 3)},
        DOWN: {2: bottom & (y < 3), 4: bottom & (y < 2), 3: bottom & (y == 0)},
    }

    def i_ref(s, half, row):
        return u[s].at[pl.ds(1 + 4 * half, 4), row, CELLS]

    def i_copy(s, way, half):
        a, b = (NI, 0) if way == I_UP else (1, NI + 1)
        return remote(i_ref(s, half, a), i_ref(s, half, b), s, way + half, to[way])

    def relay_copy(s, way):
        return remote(i_ref(s, 1, NI if way == I_UP else 1), held.at[s], s, RELAY, via)

    def forward_copy(s, way):
        return remote(held.at[s], i_ref(s, 1, 0 if way == I_UP else NI + 1), s, FORWARD, onward, way + 1)

    relayed = {I_UP: col == 1, I_DOWN: col == 2}
    forwards = {I_UP: col == 0, I_DOWN: col == 3}
    direct = {I_UP: (col == 0) | (col == 2), I_DOWN: (col == 1) | (col == 3)}

    far = {I_UP: col == 1, I_DOWN: col == 2}

    def each_i(s, act, near=True, beyond=True):
        if near:
            for way in (I_UP, I_DOWN):
                pl.when(relayed[way])(lambda way=way: act(relay_copy(s, way)))
        for way in (I_UP, I_DOWN):
            if near:
                pl.when(direct[way])(lambda way=way: [act(i_copy(s, way, half)) for half in (0, 1)] and None)
            if beyond:
                pl.when(far[way])(lambda way=way: act(i_copy(s, way, 0)))

    def forward(s):
        for way in (I_UP, I_DOWN):

            @pl.when(forwards[way])
            def _(way=way):
                relay_copy(s, way).wait_recv()
                forward_copy(s, way).start()

    def k_copy(s, g):
        start, n = PIECES[g]
        rows = pl.ds(start, n)
        return remote(kf.at[s, rows], kh.at[s, rows], s, KF + g, {"slabs": 1 - slab})

    def take_k(s, groups):
        def body(i):
            for j in range(NJ):
                kf[s, i, pl.ds(j, 1), :] = u[s][j + 1, i + 1, pl.ds(face_row, 1), :]

        rows_of(groups, body)

    def put_k(s, groups):
        def body(i):
            for j in range(NJ):
                u[s][j + 1, i + 1, pl.ds(halo_row, 1), :] = kh[s, i, pl.ds(j, 1), :]

        rows_of(groups, body)

    def each_j(s, gs, act):
        for g in gs:
            for way in (UP, DOWN):
                straight = has[way]
                if g in DETOUR:
                    straight = straight & jnp.logical_not(detours[way][g])
                    pl.when(detours[way][g])(lambda way=way, g=g: act(j_relay(s, way, g)))
                pl.when(straight)(lambda way=way, g=g: act(j_copy(s, way, g)))

    def pass_j(s, gs):
        for g in gs:
            for way in (UP, DOWN):

                @pl.when(passes[way][g])
                def _(way=way, g=g):
                    j_relay(s, way, g).wait_recv()
                    j_onward(s, way, g).start()

    def send_i(s, **which):
        each_i(s, lambda copy: copy.start(), **which)

    def send_k(s, gs):
        for g in gs:
            k_copy(s, g).start()

    def recv_i(s):
        for way, back in ((I_UP, I_DOWN), (I_DOWN, I_UP)):

            @pl.when(has[back])
            def _(way=way):
                i_copy(s, way, 0).wait_recv()
                i_copy(s, way, 1).wait_recv()

    def recv_j(s, gs):
        for g in gs:
            for way, back in ((UP, DOWN), (DOWN, UP)):

                @pl.when(has[back])
                def _(way=way, g=g):
                    j_copy(s, way, g).wait_recv()

    def recv_k(s, gs):
        for g in gs:
            k_copy(s, g).wait_recv()

    def march(s, groups):
        b = u[s]

        def body(i):
            for k in range(0, NK, 8):
                here, lower, upper = pl.ds(K0 + k, 8), pl.ds(K0 + k - 1, 8), pl.ds(K0 + k + 1, 8)
                prev, mid = b[0, i + 1, here, :], b[1, i + 1, here, :]
                for j in range(1, NJ + 1):
                    following = b[j + 1, i + 1, here, :]
                    near = (prev + following) + (b[j, i, here, :] + b[j, i + 2, here, :])
                    near = near + (b[j, i + 1, lower, :] + b[j, i + 1, upper, :])
                    new = mid * (0.6 - 0.2 * (mid * c[j - 1, i, pl.ds(k, 8), :])) + 0.1 * near
                    if s + 1 < STEPS:
                        u[s + 1][j, i + 1, here, :] = new
                    else:
                        out[j - 1, i, pl.ds(k, 8), :] = new
                    prev, mid = mid, following

        rows_of(groups, body)

    first = jnp.where(r == 0, 0.1, 0.0).astype(F32)
    later = jnp.where(r == 0, 0.0, 0.1).astype(F32)

    k_main = pl.multiple_of(8 * slab, 8)
    k_edge = pl.multiple_of(NK - 8 - (NK - 8) * slab, 8)

    def block_totals(groups, tiles):
        b = u[2]

        def body(i):
            for k in tiles:
                here, lower, upper = pl.ds(K0 + k, 8), pl.ds(K0 + k - 1, 8), pl.ds(K0 + k + 1, 8)
                own, near = None, None
                for j in range(1, NJ + 1):
                    mid = b[j, i + 1, here, :]
                    term = mid * (0.8 - 0.2 * (mid * c[j - 1, i, pl.ds(k, 8), :]))
                    if j == 1:
                        term = term - first * mid
                    beside = (b[j, i, here, :] + b[j, i + 2, here, :]) + (b[j, i + 1, lower, :] + b[j, i + 1, upper, :])
                    own = term if own is None else own + term
                    near = beside if near is None else near + beside
                tot[i, pl.ds(k, 8), :] = own + 0.1 * near

        rows_of(groups, body)

    def p_copy(n, src, dst, device):
        return pltpu.make_async_remote_copy(src, dst, ps_sem.at[n], pr_sem.at[n], device_id=device, device_id_type=MESH)

    all_k, main, edge = pl.ds(0, NK), pl.ds(k_main, NK - 8), pl.ds(k_edge, 8)
    main_tiles = [pl.multiple_of(k_main + 8 * t, 8) for t in range(NK // 8 - 1)]
    pieces = ((1, 12, 3, main), (4, 10, 2, main), (6, 8, 2, main), (1, 8, 7, edge), (0, 15, 1, all_k))
    parts = [(a + (b - a) * core, n, k) for a, b, n, k in pieces]
    parts_p = [(b + (a - b) * core, n, k) for a, b, n, k in pieces]

    def at(ref, part):
        start, n, k = part
        return ref.at[pl.ds(start, n), k]

    def t_copy(n):
        part = ((1, 3, main), (12, 3, main), (4, 8, main), (1, 14, edge), (0, 1, all_k), (15, 1, all_k))[n]
        return p_copy(n, at(tot, part), at(tot_p, part), other_core)

    def y_copy(n):
        return p_copy(6 + n, at(x_out, parts[n]), at(x_in, parts[n]), {"rows": r + 4})

    def far_copy(n, d):
        return p_copy(6 + 3 * CHUNKS + 3 * (n - 3) + d - 1, at(chip, parts[n]), at(from_y.at[d - 1], parts[n]), {"rows": r + 4 * d})

    def x_copy(n, src):
        return p_copy(6 + CHUNKS + n, at(src, parts[n]), at(p_in, parts[n]), other_chip)

    def z_copy(n, mine=True):
        part = (parts if mine else parts_p)[n]
        return p_copy(6 + 2 * CHUNKS + n, at(z, part), at(z_p, part), other_core)

    def over(part, body):
        start, n, k = part
        rows_of(((start, n),), lambda i: body(i, k))

    sends_x = ((x_lo == 0), (x_lo == 1) & (y > 0))
    takes_x = (x_lo == 1) | (y > 0)

    def chain(n):
        @pl.when(y > 0)
        def _():
            y_copy(n).wait_recv()

            def body(i, k):
                x_out[i, k, :] = x_in[i, k, :] + (tot[i, k, :] + tot_p[i, k, :])

            over(parts[n], body)

        @pl.when(y == 0)
        def _():
            def body(i, k):
                x_out[i, k, :] = tot[i, k, :] + tot_p[i, k, :]

            over(parts[n], body)

        pl.when(y < 3)(lambda: y_copy(n).start())
        pair_sends(n)

    def pair_sends(n):
        pl.when(sends_x[0])(lambda: x_copy(n, x_out).start())
        pl.when(sends_x[1])(lambda: x_copy(n, x_in).start())

    def spread(n):
        def body(i, k):
            chip[i, k, :] = tot[i, k, :] + tot_p[i, k, :]

        over(parts[n], body)
        for d in (1, 2, 3):
            pl.when(y + d < 4)(lambda d=d: far_copy(n, d).start())

    def gather(n):
        for d in (1, 2, 3):

            @pl.when(y >= d)
            def _(d=d):
                far_copy(n, d).wait_recv()

                def body(i, k):
                    x_in[i, k, :] = from_y[0, i, k, :] if d == 1 else x_in[i, k, :] + from_y[d - 1, i, k, :]

                over(parts[n], body)

        def body(i, k):
            x_out[i, k, :] = chip[i, k, :] + x_in[i, k, :]

        pl.when(y > 0)(lambda: over(parts[n], body))

        def alone(i, k):
            x_out[i, k, :] = chip[i, k, :]

        pl.when(y == 0)(lambda: over(parts[n], alone))
        pair_sends(n)

    def combine(n):
        @pl.when(takes_x)
        def _():
            x_copy(n, x_out).wait_recv()

        @pl.when(y > 0)
        def _():
            def body(i, k):
                z[i, k, :] = x_in[i, k, :] + p_in[i, k, :]

            over(parts[n], body)

        @pl.when((y == 0) & (x_lo == 1))
        def _():
            def body(i, k):
                z[i, k, :] = p_in[i, k, :]

            over(parts[n], body)

        @pl.when((y == 0) & (x_lo == 0))
        def _():
            def body(i, k):
                z[i, k, :] = jnp.zeros((8 if n == 3 else NK if n == 4 else NK - 8, NL), F32)

            over(parts[n], body)

        z_copy(n).start()

    pl.semaphore_wait(barrier, count)

    @pl.when(slab == 1)
    def _():
        pl.semaphore_signal(go_sem.at[0], 1, device_id=over_slab, device_id_type=MESH)

    @pl.when(col == 2)
    def _():
        pl.semaphore_signal(go_sem.at[1], 1, device_id=to[I_DOWN], device_id_type=MESH)
        pl.semaphore_signal(go_sem.at[1], 1, device_id=onward, device_id_type=MESH)

    load_u.wait()
    send_i(0, beyond=False)
    each_j(0, WAVES[0], lambda copy: copy.start())
    take_k(0, ((0, NI),))
    pl.when(col < 2)(lambda: pl.semaphore_wait(go_sem.at[1], 1))
    send_i(0, near=False)
    forward(0)
    pl.when(slab == 0)(lambda: pl.semaphore_wait(go_sem.at[0], 1))
    for wave in WAVES:
        send_k(0, wave)
    each_j(0, WAVES[1], lambda copy: copy.start())
    pass_j(0, (2, 3))
    each_j(0, WAVES[2], lambda copy: copy.start())
    pass_j(0, (4,))
    load_c.wait()

    for s in range(STEPS):
        if s == 2:
            block_totals(((4, 8),), main_tiles)
            t_copy(2).start()
            pl.when(y > 0)(lambda: chain(0))
            t_copy(2).wait_recv()
            pass_j(2, (4,))
            chain(1)
            chain(2)
            for wave in WAVES:
                recv_k(2, wave)
            put_k(2, PIECES)
            block_totals(((1, 14),), [k_edge])
            t_copy(3).start()
            t_copy(3).wait_recv()
            spread(3)
            recv_i(2)
            block_totals(((0, 1), (15, 1)), range(0, NK, 8))
            for n in (4, 5):
                t_copy(n).start()
            for n in (4, 5):
                t_copy(n).wait_recv()
            spread(4)
            gather(3)
            gather(4)
        for n, wave in enumerate(WAVES):
            rows = [PIECES[g] for g in wave]
            if s < 2:
                recv_k(s, wave)
                put_k(s, rows)
                if n == 0:
                    recv_i(s)
            recv_j(s, wave)
            if s == 1 and n == 0:
                pass_j(1, (4,))
            march(s, rows)
            if s < 2:
                if n == 0:
                    send_i(s + 1)
                take_k(s + 1, rows)
                send_k(s + 1, wave)
                each_j(s + 1, wave, lambda copy: copy.start())
                if n == 1:
                    forward(s + 1)
                    if s == 1:
                        block_totals(((1, 3), (12, 3)), main_tiles)
                        t_copy(0).start()
                        t_copy(1).start()
                    if s == 1:
                        t_copy(0).wait_recv()
                        t_copy(1).wait_recv()
                        pl.when(y == 0)(lambda: chain(0))
                elif n == 2:
                    pass_j(s + 1, (2, 3))

    for n in range(CHUNKS):
        combine(n)

    def finish(part, src):
        def body(i, k):
            cells = pl.ds(pl.multiple_of(K0 + k.start, 8), k.size)
            extra = later * (u2[1, i + 1, cells, :] - u2[0, i + 1, cells, :])
            below[i, k, :] = src[i, k, :] + (extra + jnp.where(core == 1, tot_p[i, k, :], 0.0))

        over(part, body)

    for n in range(CHUNKS):
        finish(parts[n], z)
    for n in range(CHUNKS):
        z_copy(n, mine=False).wait_recv()
        finish(parts_p[n], z_p)

    for s in range(STEPS):
        each_j(s, range(6), lambda copy: copy.wait_send())
        for g in DETOUR:
            for way in (UP, DOWN):
                pl.when(passes[way][g])(lambda way=way, g=g, s=s: j_onward(s, way, g).wait_send())
        each_i(s, lambda copy: copy.wait_send())
        for way in (I_UP, I_DOWN):
            pl.when(forwards[way])(lambda way=way, s=s: forward_copy(s, way).wait_send())
        for g in range(6):
            k_copy(s, g).wait_send()
    for n in range(6):
        t_copy(n).wait_send()
    for n in range(CHUNKS):
        z_copy(n).wait_send()
        if n < 3:
            pl.when(y < 3)(lambda n=n: y_copy(n).wait_send())
        else:
            for d in (1, 2, 3):
                pl.when(y + d < 4)(lambda n=n, d=d: far_copy(n, d).wait_send())
        pl.when(sends_x[0] | sends_x[1])(lambda n=n: x_copy(n, x_out).wait_send())


def write_kernel(v, below, pot, end, pot_v, sem):
    copies = [pltpu.make_async_copy(v, end, sem.at[0])]
    copies[0].start()
    for q in range(4):

        def body(i, _):
            for k in range(0, NK, 8):
                here = pl.ds(k, 8)
                total = below[i, here, :]
                for j in range(NJ):
                    total = total + v[j, i, here, :]
                    pot_v[j, i, here, :] = total * (1.0 / 128.0)
            return 0

        lax.fori_loop(4 * q, 4 * q + 4, body, 0)
        rows = pl.ds(4 * q, 4)
        copy = pltpu.make_async_copy(pot_v.at[:, rows], pot.at[:, rows], sem.at[1 + q])
        copy.start()
        copies.append(copy)
    for copy in copies:
        copy.wait()


def on_device(field_values, crowding):
    block = (NJ, NI, NK, NL)
    plane = (NI, NK, NL)
    padded = (NJ + 2, NI + 2, NK + 16, NL)
    vmem = pl.BlockSpec(memory_space=pltpu.VMEM)
    hbm = pl.BlockSpec(memory_space=pltpu.HBM)
    sems = pltpu.SemaphoreType.DMA
    out, below = pl.pallas_call(
        exchange_kernel,
        out_shape=(pltpu.VMEM(block, F32), pltpu.VMEM(plane, F32)),
        in_specs=[hbm, hbm],
        out_specs=(vmem, vmem),
        scratch_shapes=[pltpu.VMEM(padded, F32)] * 3
        + [pltpu.VMEM(block, F32)]
        + [pltpu.VMEM((STEPS, NI, NJ, NL), F32)] * 2
        + [pltpu.VMEM((STEPS, 4, NK, NL), F32), pltpu.VMEM((STEPS, len(DETOUR), 4, NK, NL), F32)]
        + [pltpu.VMEM(plane, F32)] * 8
        + [pltpu.VMEM((3,) + plane, F32)]
        + [sems((2,)), pltpu.SemaphoreType.REGULAR((2,)), sems((STEPS, N_SEM)), sems((STEPS, N_SEM)), sems((12 + 3 * CHUNKS,)), sems((12 + 3 * CHUNKS,))],
        compiler_params=pltpu.CompilerParams(collective_id=1, has_side_effects=True, vmem_limit_bytes=57 * 2**20),
        name="exchange",
    )(field_values, crowding)
    full = jax.ShapeDtypeStruct(block, F32)
    return pl.pallas_call(
        write_kernel,
        out_shape=(full, full),
        in_specs=[vmem, vmem],
        out_specs=(hbm, hbm),
        scratch_shapes=[pltpu.VMEM(block, F32), sems((5,))],
        compiler_params=pltpu.CompilerParams(vmem_limit_bytes=16 * 2**20),
        name="write",
    )(out, below)


def solution(mesh):
    spec = P(("trial", "rows"), "cols", "slabs", None)
    return jax.shard_map(on_device, mesh=mesh, in_specs=(spec, spec), out_specs=(spec, spec), check_vma=False)
```
